32 devices in a mesh: depth: 4 (over y, core), hx: 4 (over z), hy: 2 (over x).
Axes of the slice: x: 2, y: 2, z: 4, core: 2. Of those that a mesh axis runs over, the one named last changes fastest.
Arguments:
- fine_velocity: float32 [3, 16, 24, 768], P(None, 'depth', 'hx', 'hy'), may hold values from -6 to 6
- fine_stress: float32 [6, 16, 24, 768], P(None, 'depth', 'hx', 'hy'), may hold values from -3 to 3
- coarse_velocity: float32 [3, 8, 8, 256], P(None, 'depth', 'hx', 'hy'), may hold values from -6 to 6
- coarse_stress: float32 [6, 8, 8, 256], P(None, 'depth', 'hx', 'hy'), may hold values from -3 to 3
- iwan_states: float32 [10, 6, 16, 24, 768], P(None, None, 'depth', 'hx', 'hy'), may hold values from -0.3 to 0.3
- fine_zones: int32 [16, 24, 768], P('depth', 'hx', 'hy'), may hold values from 0 to 15
- coarse_zones: int32 [8, 8, 256], P('depth', 'hx', 'hy'), may hold values from 0 to 15
- plastic: int32 [16, 24, 768], P('depth', 'hx', 'hy'), may hold values from 0 to 1, as said below
- zone_buoyancy: float32 [16], replicated, may hold values from 0.5 to 1
- zone_lambda: float32 [16], replicated, may hold values from 0.1 to 0.3
- zone_mu: float32 [16], replicated, may hold values from 0.1 to 0.3
- iwan_share: float32 [10], replicated, may hold values from 0.3 to 3
- iwan_radius: float32 [10], replicated, may hold values from 0.01 to 0.3
Outputs:
- fine_velocity_out: float32 [3, 16, 24, 768], P(None, 'depth', 'hx', 'hy')
- fine_stress_out: float32 [6, 16, 24, 768], P(None, 'depth', 'hx', 'hy')
- coarse_velocity_out: float32 [3, 8, 8, 256], P(None, 'depth', 'hx', 'hy')
- coarse_stress_out: float32 [6, 8, 8, 256], P(None, 'depth', 'hx', 'hy')
The draws below stay inside these ranges and needn't reach their ends.
Inputs may be any that keep to these rules, and one draw needn't show every extreme that they name: `plastic`: 1 marks a cell that follows the Iwan model, 0 an elastic cell.
All inputs are finite; a program needn't handle non-finite values.
Results may differ from the reference program's by a relative error of at most 0.0001.
Values sent between devices are 32-bit elements; how exact they have to be, the bound alone decides.
A program may use at most 64 MiB of HBM per device.

```python
import math
import jax
import jax.numpy as jnp
from jax import lax

STEPS = 2
SURF = 10
ZONES = 16
NX = 24
NY = 768
NZF = 16
NXC = 8
NYC = 256
NZC = 8


def draw_plastic(key, part):
    first_key, second_key = jax.random.split(jax.random.fold_in(key, 17))
    fault = jax.random.randint(first_key, (), 0, NX)
    columns = jnp.arange(NX, dtype=jnp.int32)
    distance = jnp.abs(columns - fault)
    limits = jnp.maximum(0, 48 - 2 * distance)
    levels = jax.random.randint(second_key, (NZF, NX, NY), 0, 64)
    return (levels < limits[None, :, None]).astype(jnp.int32)


def with_ends(entries, own_key, low, high):
    shape = entries.shape
    spot = [jax.random.randint(jax.random.fold_in(own_key, axis), (), 0, shape[axis]) for axis in range(len(shape))]
    entries = entries.at[tuple(spot)].set(low)
    longest = shape.index(max(shape))
    spot[longest] = (spot[longest] + 1) % shape[longest]
    return entries.at[tuple(spot)].set(high)


def shard_levels(own_key, shape, pieces, least, high):
    gain, own = 1.0, jax.random.fold_in(own_key, 6)
    for axis_at, shards_of in pieces:
        steps = jnp.exp(jax.random.uniform(jax.random.fold_in(own, axis_at), (shards_of,), jnp.float32, least / len(pieces), high / len(pieces)))
        gain = gain * jnp.repeat(steps, shape[axis_at] // shards_of).reshape([-1 if axis == axis_at else 1 for axis in range(len(shape))])
    return gain


def noise(key, shape, scale, most, pieces=(), held_as=jnp.bfloat16):
    gain = shard_levels(key, shape, pieces, -0.22, 0.18) if pieces else 1.0
    values = jax.random.normal(key, shape, jnp.float32) * scale * gain
    return jnp.minimum(jnp.maximum(values, -most), most).astype(held_as)


def setup_inputs(seed: int = 0) -> dict:
    key_list = jax.random.split(jax.random.key(seed), 14)
    fine_velocity = noise(key_list[0], (3, NZF, NX, NY), 1.0, 6.0, ((1, 4), (2, 4), (3, 2)), jnp.float32)
    fine_stress = noise(key_list[1], (6, NZF, NX, NY), 0.5, 3.0, ((1, 4), (2, 4), (3, 2)), jnp.float32)
    coarse_velocity = noise(key_list[2], (3, NZC, NXC, NYC), 1.0, 6.0, ((1, 4), (2, 4), (3, 2)), jnp.float32)
    coarse_stress = noise(key_list[3], (6, NZC, NXC, NYC), 0.5, 3.0, ((1, 4), (2, 4), (3, 2)), jnp.float32)
    iwan_states = noise(key_list[4], (SURF, 6, NZF, NX, NY), 0.05, 0.3, ((2, 4), (3, 4), (4, 2)), jnp.float32)
    fine_zones = with_ends(jax.random.randint(key_list[5], (NZF, NX, NY), 0, ZONES), jax.random.fold_in(key_list[5], 1), 0, ZONES - 1).astype(jnp.int32)
    coarse_zones = with_ends(jax.random.randint(key_list[6], (NZC, NXC, NYC), 0, ZONES), jax.random.fold_in(key_list[6], 1), 0, ZONES - 1).astype(jnp.int32)
    plastic = draw_plastic(jax.random.fold_in(key_list[13], 71), 0)
    zone_buoyancy = jnp.clip(jax.random.uniform(key_list[8], (ZONES,), jnp.float32, 0.5, 1.0), 0.5, 1.0)
    zone_lambda = jnp.clip(jax.random.uniform(key_list[9], (ZONES,), jnp.float32, 0.1, 0.3), 0.1, 0.3)
    zone_mu = jnp.clip(jax.random.uniform(key_list[10], (ZONES,), jnp.float32, 0.1, 0.3), 0.1, 0.3)
    iwan_share = jnp.clip(jnp.exp(jax.random.uniform(key_list[11], (SURF,), jnp.float32, math.log(0.3), math.log(3.0))), 0.3, 3.0)
    iwan_radius = jnp.clip(jnp.exp(jax.random.uniform(key_list[12], (SURF,), jnp.float32, math.log(0.01), math.log(0.3))), 0.01, 0.3)
    return dict(fine_velocity=fine_velocity, fine_stress=fine_stress, coarse_velocity=coarse_velocity, coarse_stress=coarse_stress, iwan_states=iwan_states, fine_zones=fine_zones, coarse_zones=coarse_zones, plastic=plastic, zone_buoyancy=zone_buoyancy, zone_lambda=zone_lambda, zone_mu=zone_mu, iwan_share=iwan_share, iwan_radius=iwan_radius)


step_time = 0.4
near_coef = 9.0 / 8.0
far_coef = 1.0 / 24.0

def shifted(padded, along, offset):
    length = padded.shape[along] - 4
    return lax.slice_in_dim(padded, 2 + offset, 2 + offset + length, axis=along)

def derivative(padded, along, forward, spacing):
    if forward:
        value = near_coef * (shifted(padded, along, 1) - shifted(padded, along, 0)) - far_coef * (shifted(padded, along, 2) - shifted(padded, along, -1))
    else:
        value = near_coef * (shifted(padded, along, 0) - shifted(padded, along, -1)) - far_coef * (shifted(padded, along, 1) - shifted(padded, along, -2))
    return value / spacing

def inner(padded, dims):
    for other in dims:
        padded = lax.slice_in_dim(padded, 2, padded.shape[other] - 2, axis=other)
    return padded

def lookup(zone_ids, values):
    total = jnp.zeros(zone_ids.shape, jnp.float32)
    for member in range(values.shape[0]):
        total = total + jnp.where(zone_ids == member, values[member], jnp.float32(0.0))
    return total

def spread(plane):
    return jnp.repeat(jnp.repeat(plane, 3, axis=-2), 3, axis=-1)

def shrink(plane):
    shape = plane.shape
    return plane.reshape(shape[:-2] + (shape[-2] // 3, 3, shape[-1] // 3, 3)).mean(axis=(-3, -1))

def whole_getter(padded):

    def getter(component, along):
        return inner(padded[component], [other for other in (0, 1, 2) if other != along])
    return getter

def velocity_step(velocity, getter, buoyancy, spacing):
    force_x = derivative(getter(0, 1), 1, True, spacing) + derivative(getter(3, 2), 2, False, spacing) + derivative(getter(4, 0), 0, False, spacing)
    force_y = derivative(getter(3, 1), 1, False, spacing) + derivative(getter(1, 2), 2, True, spacing) + derivative(getter(5, 0), 0, False, spacing)
    force_z = derivative(getter(4, 1), 1, False, spacing) + derivative(getter(5, 2), 2, False, spacing) + derivative(getter(2, 0), 0, True, spacing)
    return velocity + step_time * buoyancy[None] * jnp.stack([force_x, force_y, force_z])

def strain_rates(padded, spacing):
    getter = whole_getter(padded)

    def rate(component, along, forward):
        return derivative(getter(component, along), along, forward, spacing)
    rate_xx = rate(0, 1, False)
    rate_yy = rate(1, 2, False)
    rate_zz = rate(2, 0, False)
    rate_xy = rate(1, 1, True) + rate(0, 2, True)
    rate_xz = rate(2, 1, True) + rate(0, 0, True)
    rate_yz = rate(2, 2, True) + rate(1, 0, True)
    return [rate_xx, rate_yy, rate_zz, rate_xy, rate_xz, rate_yz]

def elastic_stress(stress, rates, lame_first, shear_mod):
    dilation = rates[0] + rates[1] + rates[2]
    normal = [stress[member] + step_time * (lame_first * dilation + 2.0 * shear_mod * rates[member]) for member in range(3)]
    shear = [stress[member] + step_time * shear_mod * rates[member] for member in range(3, 6)]
    return jnp.stack(normal + shear)

def deviator_increment(rates, shear_mod):
    dilation = rates[0] + rates[1] + rates[2]
    normal = [2.0 * shear_mod * step_time * (rates[member] - dilation / 3.0) for member in range(3)]
    shear = [shear_mod * step_time * rates[member] for member in range(3, 6)]
    return jnp.stack(normal + shear)

def plastic_stress(stress, rates, lame_first, shear_mod, deviator):
    dilation = rates[0] + rates[1] + rates[2]
    mean_part = (stress[0] + stress[1] + stress[2]) / 3.0 + step_time * (lame_first + 2.0 * shear_mod / 3.0) * dilation
    return jnp.stack([mean_part + deviator[0], mean_part + deviator[1], mean_part + deviator[2], deviator[3], deviator[4], deviator[5]])

def iwan_return(states, increment, weights, radius):
    trial_state = states + weights[:, None, None, None, None] * increment[None]
    magnitude = jnp.sqrt(0.5 * (trial_state[:, 0] ** 2 + trial_state[:, 1] ** 2 + trial_state[:, 2] ** 2) + trial_state[:, 3] ** 2 + trial_state[:, 4] ** 2 + trial_state[:, 5] ** 2)
    limits = radius[:, None, None, None]
    scaled = trial_state * (limits / jnp.maximum(magnitude, limits))[:, None]
    return (scaled, lax.optimization_barrier(jnp.sum(scaled, axis=0)))

def attach_below(padded, rows, ghosts, flag, margin):
    depth_len = padded.shape[1]
    picks = jnp.array(rows, dtype=jnp.int32)
    for offset in range(2):
        old = padded[picks, depth_len - 2 + offset, margin:padded.shape[2] - margin, margin:padded.shape[3] - margin]
        padded = padded.at[picks, depth_len - 2 + offset, margin:padded.shape[2] - margin, margin:padded.shape[3] - margin].set(jnp.where(flag, ghosts[offset], old))
    return padded

def attach_above(padded, rows, ghosts, flag, margin):
    picks = jnp.array(rows, dtype=jnp.int32)
    for offset in range(2):
        old = padded[picks, 1 - offset, margin:padded.shape[2] - margin, margin:padded.shape[3] - margin]
        padded = padded.at[picks, 1 - offset, margin:padded.shape[2] - margin, margin:padded.shape[3] - margin].set(jnp.where(flag, ghosts[offset], old))
    return padded

def pad_all(stack):
    return jnp.pad(stack, ((0, 0), (2, 2), (2, 2), (2, 2)))

def join_grids(fine_pad, coarse_pad, fine_full, coarse_full, rows):
    picks = jnp.array(rows, dtype=jnp.int32)
    fine_rows = fine_full[picks]
    coarse_rows = coarse_full[picks]
    below = spread(coarse_rows[:, 0])
    bottom = fine_rows[:, -1]
    ghosts = [2.0 / 3.0 * bottom + 1.0 / 3.0 * below, 1.0 / 3.0 * bottom + 2.0 / 3.0 * below]
    above = shrink(jnp.stack([fine_rows[:, -1], fine_rows[:, -4]]))
    fine_pad = attach_below(fine_pad, rows, ghosts, True, 2)
    coarse_pad = attach_above(coarse_pad, rows, above, True, 2)
    return (fine_pad, coarse_pad)

def reference(fine_velocity, fine_stress, coarse_velocity, coarse_stress, iwan_states, fine_zones, coarse_zones, plastic, zone_buoyancy, zone_lambda, zone_mu, iwan_share, iwan_radius):
    coarse_velocity = jnp.flip(coarse_velocity, 1)
    coarse_stress = jnp.flip(coarse_stress, 1)
    coarse_zones = jnp.flip(coarse_zones, 0)
    fine_buoyancy = lookup(fine_zones, zone_buoyancy)
    fine_lame = lookup(fine_zones, zone_lambda)
    fine_shear = lookup(fine_zones, zone_mu)
    coarse_buoyancy = lookup(coarse_zones, zone_buoyancy)
    coarse_lame = lookup(coarse_zones, zone_lambda)
    coarse_shear = lookup(coarse_zones, zone_mu)
    weights = iwan_share / jnp.sum(iwan_share)
    active = plastic == 1
    states = iwan_states
    for step in range(STEPS):
        fine_pad, coarse_pad = join_grids(pad_all(fine_stress), pad_all(coarse_stress), fine_stress, coarse_stress, (2, 4, 5))
        fine_velocity = velocity_step(fine_velocity, whole_getter(fine_pad), fine_buoyancy, 1.0)
        coarse_velocity = velocity_step(coarse_velocity, whole_getter(coarse_pad), coarse_buoyancy, 3.0)
        fine_pad, coarse_pad = join_grids(pad_all(fine_velocity), pad_all(coarse_velocity), fine_velocity, coarse_velocity, (0, 1, 2))
        fine_rates = strain_rates(fine_pad, 1.0)
        elastic = elastic_stress(fine_stress, fine_rates, fine_lame, fine_shear)
        increment = deviator_increment(fine_rates, fine_shear)

        def plane_update(member, carry):
            states_now, deviator_now = carry
            part_states = lax.dynamic_slice_in_dim(states_now, member, 1, 2)
            part_increment = lax.dynamic_slice_in_dim(increment, member, 1, 1)
            part_active = lax.dynamic_slice_in_dim(active, member, 1, 0)
            scaled, deviator = iwan_return(part_states, part_increment, weights, iwan_radius)
            kept = jnp.where(part_active[None, None], scaled, part_states)
            states_now = lax.dynamic_update_slice_in_dim(states_now, kept, member, 2)
            deviator_now = lax.dynamic_update_slice_in_dim(deviator_now, deviator, member, 1)
            return (states_now, deviator_now)
        states, deviator_all = lax.fori_loop(0, fine_stress.shape[1], plane_update, (states, jnp.zeros_like(increment)))
        yielded = plastic_stress(fine_stress, fine_rates, fine_lame, fine_shear, deviator_all)
        fine_stress = jnp.where(active[None], yielded, elastic)
        coarse_rates = strain_rates(coarse_pad, 3.0)
        coarse_stress = elastic_stress(coarse_stress, coarse_rates, coarse_lame, coarse_shear)
    return (fine_velocity, fine_stress, jnp.flip(coarse_velocity, 1), jnp.flip(coarse_stress, 1))
```

```python
import jax
import jax.numpy as jnp
from jax import lax
from jax.experimental import pallas as pl
from jax.experimental.pallas import tpu as pltpu
from jax.sharding import PartitionSpec as P

STEPS = 2
DT = 0.4
NEAR = 9.0 / 8.0
FAR = 1.0 / 24.0
MESH = pl.DeviceIdType.MESH
Z_PARTS, X_PARTS, Y_PARTS = (2, 4, 5), (0, 3, 4), (1, 3, 5)
AXES = ("depth", "hx", "hy")


class Grid:
    def __init__(self, shape, spacing, flipped):
        self.nz, self.nx, self.ny = shape
        self.near, self.far = NEAR / spacing, FAR / spacing
        self.flipped = flipped

    def at(self, z):
        return self.nz - 1 - z if self.flipped else z


def roll(x, amount, axis):
    return pltpu.roll(x, amount % x.shape[axis], axis)


def diff_z(g, ref, c, z, forward):
    o = 2 + z + (1 if forward else 0)
    return g.near * (ref[c, o] - ref[c, o - 1]) - g.far * (ref[c, o + 1] - ref[c, o - 2])


def diff_x(g, ref, c, z, forward):
    o = 3 if forward else 2
    at = lambda s: ref[c, z, s : s + g.nx, :]
    return g.near * (at(o) - at(o - 1)) - g.far * (at(o + 1) - at(o - 2))


def diff_y(g, ref, c, z, forward):
    ext = ref[c, z]
    at = lambda s: (roll(ext, -s, 1) if s else ext)[:, : g.ny]
    o = 1 if forward else 0
    return g.near * (at(o) - at(o - 1)) - g.far * (at(o + 1) - at(o - 2))


def put_ext(g, ext, comps, z, values):
    ze, xe, ye = ext
    zc, xc, yc = comps
    for slot, c in enumerate(zc):
        ze[slot, 2 + z] = values[c]
    for slot, c in enumerate(xc):
        xe[slot, z, 2 : 2 + g.nx, :] = values[c]
    for slot, c in enumerate(yc):
        ye[slot, z, :, : g.ny] = values[c]


def pack(fine, coarse, fext, cext, sz, sx, sy):
    fz, fx, fy = fext
    cz, cx, cy = cext
    for c in range(3):
        for l in range(2):
            for side in range(2):
                fl = l if side == 0 else fine.nz - 2 + l
                cl = l if side == 1 else coarse.nz - 2 + l
                sz[side, 2 * c + l, 0 : fine.nx, :] = fz[c, 2 + fl]
                sz[side, 2 * c + l, fine.nx : fine.nx + coarse.nx, 0 : coarse.ny] = cz[c, 2 + cl]
        for g, ext in ((fine, fx), (coarse, cx)):
            for z in range(g.nz):
                for side in range(2):
                    first = 2 if side == 0 else g.nx
                    rows = ext[c, z, first : first + 2, :]
                    if g is fine:
                        sx[side, c, 2 * z : 2 * z + 2, :] = rows
                    else:
                        sx[side, 3, 2 * z : 2 * z + 2, c * g.ny : (c + 1) * g.ny] = rows
    for tile, (g, ext) in enumerate(((fine, fy), (coarse, cy))):
        lane = lax.broadcasted_iota(jnp.int32, (g.nx, 128), 1)
        total = jnp.zeros((g.nx, 128), jnp.float32)
        for c in range(3):
            for z in range(g.nz):
                i = c * g.nz + z
                plane = ext[c, z, :, 0:128]
                if g.ny > 128:
                    plane = jnp.where(lane < 64, plane, ext[c, z, :, g.ny - 128 : g.ny])
                total = jnp.where(lane // 4 == i, roll(plane, 4 * i + 2, 1), total)
        sy[tile, 0 : g.nx, :] = total


def unpack_z(fine, coarse, fext, cext, rz):
    for c in range(3):
        for l in range(2):
            for side in range(2):
                fext[0][c, l if side == 0 else 2 + fine.nz + l] = rz[side, 2 * c + l, 0 : fine.nx, :]
                cext[0][c, l if side == 1 else 2 + coarse.nz + l] = rz[
                    side, 2 * c + l, fine.nx : fine.nx + coarse.nx, 0 : coarse.ny
                ]


def unpack_x(fine, coarse, fext, cext, rx):
    for c in range(3):
        for g, ext in ((fine, fext[1]), (coarse, cext[1])):
            for z in range(g.nz):
                for side in range(2):
                    first = 0 if side == 0 else 2 + g.nx
                    if g is fine:
                        rows = rx[side, c, 2 * z : 2 * z + 2, :]
                    else:
                        rows = rx[side, 3, 2 * z : 2 * z + 2, c * g.ny : (c + 1) * g.ny]
                    ext[c, z, first : first + 2, :] = rows


def unpack_y(fine, coarse, fext, cext, ry):
    for tile, (g, ext) in enumerate(((fine, fext[2]), (coarse, cext[2]))):
        lane = lax.broadcasted_iota(jnp.int32, (g.nx, 128), 1)
        both = jnp.where(lane % 4 < 2, ry[0, tile, 0 : g.nx, :], ry[1, tile, 0 : g.nx, :])
        for c in range(3):
            for z in range(g.nz):
                i = c * g.nz + z
                ext[c, z, :, g.ny : g.ny + 128] = roll(both, -(4 * i + 2), 1)


def couple(fine, coarse, fext, cext):
    fz, cz = fext[0], cext[0]
    nt = fine.ny // 128
    lane = lax.broadcasted_iota(jnp.int32, (fine.nx, 128), 1)
    row = lax.broadcasted_iota(jnp.int32, (fine.nx, 128), 0)
    clane = lane[0 : coarse.nx]
    ratio = fine.ny // coarse.ny
    for c in range(3):
        bottom = fz[c, 1 + fine.nz]
        plane = cz[c, 2]
        rows = jnp.broadcast_to(plane[0:1], (fine.nx, coarse.ny))
        for r in range(1, coarse.nx):
            rows = jnp.where(row < 3 * r, rows, jnp.broadcast_to(plane[r : r + 1], rows.shape))
        spread = jnp.concatenate(
            [jnp.take_along_axis(rows, (lane + 128 * t) // 3, axis=1) for t in range(nt)], axis=1
        )
        fz[c, 2 + fine.nz] = 2.0 / 3.0 * bottom + 1.0 / 3.0 * spread
        fz[c, 3 + fine.nz] = 1.0 / 3.0 * bottom + 2.0 / 3.0 * spread
        for slot, z in ((1, fine.nz - 1), (0, fine.nz - 4)):
            f = fz[c, 2 + z]
            f = f + roll(f, -1, 1) + roll(f, -2, 1)
            sums = jnp.concatenate(
                [jnp.sum(f[3 * r : 3 * r + 3], axis=0, keepdims=True) for r in range(coarse.nx)], axis=0
            )
            out = jnp.zeros((coarse.nx, 128), jnp.float32)
            for t in range(nt):
                got = jnp.take_along_axis(sums[:, 128 * t : 128 * t + 128], (3 * clane) % 128, axis=1)
                out = jnp.where((3 * clane) // 128 == t, got, out)
            cz[c, slot] = out * (1.0 / 9.0)


def materials(g, zones, tables, out):
    def body(z, carry):
        ids = zones[g.at(z)]
        values = [jnp.zeros(ids.shape, jnp.float32)] * 3
        for member in range(tables[0].shape[0]):
            hit = ids == member
            values = [jnp.where(hit, t[member], v) for t, v in zip(tables, values)]
        out[0, z] = DT * values[0]
        out[1, z] = DT * values[1]
        out[2, z] = DT * values[2]
        return carry

    lax.fori_loop(0, g.nz, body, 0)


def velocity_update(g, sext, vext, mats, velocity):
    ze, xe, ye = sext
    allc = (0, 1, 2)

    def body(z, carry):
        b = mats[0, z]
        force = (
            diff_x(g, xe, 0, z, True) + diff_y(g, ye, 1, z, False) + diff_z(g, ze, 1, z, False),
            diff_x(g, xe, 1, z, False) + diff_y(g, ye, 0, z, True) + diff_z(g, ze, 2, z, False),
            diff_x(g, xe, 2, z, False) + diff_y(g, ye, 2, z, False) + diff_z(g, ze, 0, z, True),
        )
        new = [velocity[c, g.at(z)] + b * force[c] for c in range(3)]
        for c in range(3):
            velocity[c, g.at(z)] = new[c]
        put_ext(g, vext, (allc, allc, allc), z, new)
        return carry

    lax.fori_loop(0, g.nz, body, 0)


def stress_update(g, vext, sext, mats, stress, iwan, last):
    ze, xe, ye = vext

    def body(z, carry):
        lame, shear = mats[1, z], mats[2, z]
        exx = diff_x(g, xe, 0, z, False)
        eyy = diff_y(g, ye, 1, z, False)
        ezz = diff_z(g, ze, 2, z, False)
        exy = diff_x(g, xe, 1, z, True) + diff_y(g, ye, 0, z, True)
        exz = diff_x(g, xe, 2, z, True) + diff_z(g, ze, 0, z, True)
        eyz = diff_y(g, ye, 2, z, True) + diff_z(g, ze, 1, z, True)
        dilation = exx + eyy + ezz
        old = [stress[c, g.at(z)] for c in range(6)]
        volume = lame * dilation
        twice = 2.0 * shear
        shears = [shear * exy, shear * exz, shear * eyz]
        new = [old[c] + volume + twice * e for c, e in enumerate((exx, eyy, ezz))]
        new += [old[3 + c] + shears[c] for c in range(3)]
        if iwan is not None:
            states, plastic, share, radius, surfaces = iwan
            third = dilation * (1.0 / 3.0)
            total = share[0]
            for k in range(1, surfaces):
                total = total + share[k]
            scale = 1.0 / jnp.full(dilation.shape, total, jnp.float32)
            dd = [scale * (twice * (e - third)) for e in (exx, eyy, ezz)]
            dd += [scale * s for s in shears]
            sums = None
            for k in range(surfaces):
                t = [states[k, c, z] + share[k] * dd[c] for c in range(6)]
                j2 = 0.5 * (t[0] * t[0] + t[1] * t[1] + t[2] * t[2]) + (
                    t[3] * t[3] + t[4] * t[4] + t[5] * t[5]
                )
                factor = jnp.minimum(1.0, radius[k] * lax.rsqrt(j2))
                t = [factor * x for x in t]
                if not last:
                    for c in range(6):
                        states[k, c, z] = t[c]
                sums = t if sums is None else [a + b for a, b in zip(sums, t)]
            mean = (old[0] + old[1] + old[2]) * (1.0 / 3.0) + (lame + twice * (1.0 / 3.0)) * dilation
            active = plastic[z] == 1
            yielded = [mean + sums[c] for c in range(3)] + sums[3:]
            new = [jnp.where(active, a, b) for a, b in zip(yielded, new)]
        for c in range(6):
            stress[c, g.at(z)] = new[c]
        if not last:
            put_ext(g, sext, (Z_PARTS, X_PARTS, Y_PARTS), z, new)
        return carry

    lax.fori_loop(0, g.nz, body, 0)


def kernel(counts, fine, coarse, surfaces, *refs):
    (fv_in, fs_in, cv_in, cs_in, st_in, fzo_in, czo_in, pl_in) = refs[:8]
    tables, share, radius = refs[8:11], refs[11], refs[12]
    fv_out, fs_out, cv_out, cs_out = refs[13:17]
    (fv, fs, cv, cs, st, fzo, czo, plastic) = refs[17:25]
    fmat, cmat = refs[25:27]
    fsx, csx, fvx, cvx = refs[27:30], refs[30:33], refs[33:36], refs[36:39]
    sends, recvs = refs[39:42], refs[42:45]
    in_sem, out_sem, send_sem, recv_sem = refs[45:49]

    place = [lax.axis_index(a) for a in AXES]
    exists = lambda a, side: (place[a] > 0) if side == 0 else (place[a] < counts[a] - 1)
    peer = lambda a, side: {AXES[a]: place[a] + (1 if side else -1)}

    order = (1, 3, 0, 2, 5, 6, 7, 4)
    loads = [
        pltpu.make_async_copy(src, dst, in_sem.at[i])
        for i, (src, dst) in enumerate(zip(refs[:8], refs[17:25]))
    ]
    for i in order:
        loads[i].start()

    barrier = pltpu.get_barrier_semaphore()
    for a in range(3):
        for side in range(2):

            @pl.when(exists(a, side))
            def _():
                pl.semaphore_signal(barrier, inc=1, device_id=peer(a, side), device_id_type=MESH)

            @pl.when(jnp.logical_not(exists(a, side)))
            def _():
                for e in range(2 * STEPS):
                    recvs[a][e, side] = jnp.zeros(recvs[a].shape[2:], jnp.float32)

    def copy(e, a, side):
        src = sends[a].at[e, side] if a < 2 else sends[a].at[e]
        return pltpu.make_async_remote_copy(
            src_ref=src,
            dst_ref=recvs[a].at[e, 1 - side],
            send_sem=send_sem.at[e, a, side],
            recv_sem=recv_sem.at[e, a, 1 - side],
            device_id=peer(a, side),
            device_id_type=MESH,
        )

    def start(e):
        for a in range(3):
            for side in range(2):

                @pl.when(exists(a, side))
                def _():
                    copy(e, a, side).start()

    def arrive(e, a):
        for side in range(2):

            @pl.when(exists(a, side))
            def _():
                copy(e, a, 1 - side).wait_recv()

    loads[1].wait()
    loads[3].wait()
    for g, s, ext in ((fine, fs, fsx), (coarse, cs, csx)):
        for z in range(g.nz):
            put_ext(g, ext, (Z_PARTS, X_PARTS, Y_PARTS), z, [s[c, g.at(z)] for c in range(6)])

    at_interface = place[0] == counts[0] - 1
    for e in range(2 * STEPS):
        fext, cext = (fsx, csx) if e % 2 == 0 else (fvx, cvx)
        pack(fine, coarse, fext, cext, sends[0].at[e], sends[1].at[e], sends[2].at[e])
        if e == 0:
            neighbours = sum(
                exists(a, side).astype(jnp.int32) for a in range(3) for side in range(2)
            )
            pl.semaphore_wait(barrier, neighbours)
        start(e)
        if e == 0:
            loads[5].wait()
            loads[6].wait()
            materials(fine, fzo, tables, fmat)
            materials(coarse, czo, tables, cmat)
            loads[0].wait()
            loads[2].wait()
        arrive(e, 2)
        unpack_y(fine, coarse, fext, cext, recvs[2].at[e])
        arrive(e, 0)
        unpack_z(fine, coarse, fext, cext, recvs[0].at[e])

        @pl.when(at_interface)
        def _():
            couple(fine, coarse, fext, cext)

        arrive(e, 1)
        unpack_x(fine, coarse, fext, cext, recvs[1].at[e])
        last = e >= 2 * STEPS - 2
        if e % 2 == 0:
            velocity_update(fine, fsx, fvx, fmat, fv)
            velocity_update(coarse, csx, cvx, cmat, cv)
            if last:
                stores = [
                    pltpu.make_async_copy(fv, fv_out, out_sem.at[0]),
                    pltpu.make_async_copy(cv, cv_out, out_sem.at[1]),
                ]
                for s in stores:
                    s.start()
        else:
            if e == 1:
                loads[7].wait()
                loads[4].wait()
            stress_update(
                fine, fvx, fsx, fmat, fs, (st, plastic, share, radius, surfaces), last
            )
            stress_update(coarse, cvx, csx, cmat, cs, None, last)
    tail = [
        pltpu.make_async_copy(fs, fs_out, out_sem.at[2]),
        pltpu.make_async_copy(cs, cs_out, out_sem.at[3]),
    ]
    for s in tail:
        s.start()
    for e in range(2 * STEPS):
        for a in range(3):
            for side in range(2):

                @pl.when(exists(a, side))
                def _():
                    copy(e, a, side).wait_send()

    for s in stores + tail:
        s.wait()


def per_device(counts, *args):
    fv, fs, cv, cs, st = args[:5]
    fine = Grid(fv.shape[1:], 1.0, False)
    coarse = Grid(cv.shape[1:], 3.0, True)
    f32 = jnp.float32

    def exts(g):
        return [
            pltpu.VMEM((3, g.nz + 4, g.nx, g.ny), f32),
            pltpu.VMEM((3, g.nz, -(-(g.nx + 4) // 8) * 8, g.ny), f32),
            pltpu.VMEM((3, g.nz, g.nx, g.ny + 128), f32),
        ]

    zrows = -(-(fine.nx + coarse.nx) // 8) * 8
    xrows = -(-2 * max(fine.nz, coarse.nz) // 8) * 8
    shapes = ((6, zrows, fine.ny), (4, xrows, fine.ny), (2, 8, 128))
    phases = 2 * STEPS
    scratch = [pltpu.VMEM(a.shape, a.dtype) for a in args[:8]]
    scratch += [pltpu.VMEM((3, g.nz, g.nx, g.ny), f32) for g in (fine, coarse)]
    scratch += exts(fine) + exts(coarse) + exts(fine) + exts(coarse)
    scratch += [
        pltpu.VMEM((phases, 2) + shapes[0], f32),
        pltpu.VMEM((phases, 2) + shapes[1], f32),
        pltpu.VMEM((phases,) + shapes[2], f32),
    ]
    scratch += [pltpu.VMEM((phases, 2) + s, f32) for s in shapes]
    scratch += [
        pltpu.SemaphoreType.DMA((8,)),
        pltpu.SemaphoreType.DMA((4,)),
        pltpu.SemaphoreType.DMA((phases, 3, 2)),
        pltpu.SemaphoreType.DMA((phases, 3, 2)),
    ]
    anywhere = pl.BlockSpec(memory_space=pl.ANY)
    scalars = pl.BlockSpec(memory_space=pltpu.SMEM)
    return pl.pallas_call(
        lambda *refs: kernel(counts, fine, coarse, st.shape[0], *refs),
        name="waves",
        out_shape=[jax.ShapeDtypeStruct(a.shape, a.dtype) for a in (fv, fs, cv, cs)],
        in_specs=[anywhere] * 8 + [scalars] * 5,
        out_specs=[anywhere] * 4,
        scratch_shapes=scratch,
        compiler_params=pltpu.CompilerParams(collective_id=0, has_side_effects=True),
    )(*args)


def solution(mesh):
    field = P(None, *AXES)
    cells = P(*AXES)
    counts = tuple(mesh.shape[a] for a in AXES)
    return jax.shard_map(
        lambda *args: tuple(per_device(counts, *args)),
        mesh=mesh,
        in_specs=(field,) * 4 + (P(None, None, *AXES),) + (cells,) * 3 + (P(),) * 5,
        out_specs=(field,) * 4,
        check_vma=False,
    )
```

```python
import jax
import jax.numpy as jnp
from jax import lax
from jax.experimental import pallas as pl
from jax.experimental.pallas import tpu as pltpu
from jax.sharding import PartitionSpec as P

STEPS = 2
DT = 0.4
NEAR = 9.0 / 8.0
FAR = 1.0 / 24.0
MESH = pl.DeviceIdType.MESH
Z_PARTS, X_PARTS, Y_PARTS = (2, 4, 5), (0, 3, 4), (1, 3, 5)
AXES = ("depth", "hx", "hy")


class Grid:
    def __init__(self, shape, spacing, flipped, lead):
        self.lead, self.sub, self.ny = shape
        self.near, self.far = NEAR / spacing, FAR / spacing
        self.flipped = flipped
        self.lead_axis = lead

    def at(self, n):
        return self.lead - 1 - n if self.flipped else n


def roll(x, amount, axis):
    return pltpu.roll(x, amount % x.shape[axis], axis)


def diff(g, axis, ext, c, n, forward):
    ref = ext[axis]
    if axis == 2:
        full = ref[c, n]
        at = lambda s: (roll(full, -s, 1) if s else full)[:, : g.ny]
        o = 0
    elif axis == g.lead_axis:
        at = lambda s: ref[c, s]
        o = 2 + n
    else:
        at = lambda s: ref[c, n, s : s + g.sub, :]
        o = 2
    o = o + 1 if forward else o
    return g.near * (at(o) - at(o - 1)) - g.far * (at(o + 1) - at(o - 2))


def put_ext(g, ext, comps, n, values):
    for axis in range(3):
        for slot, c in enumerate(comps[axis]):
            if axis == 2:
                ext[axis][slot, n, :, : g.ny] = values[c]
            elif axis == g.lead_axis:
                ext[axis][slot, 2 + n] = values[c]
            else:
                ext[axis][slot, n, 2 : 2 + g.sub, :] = values[c]


def pack_sub(g, ext, out):
    ref = ext[1 - g.lead_axis]
    for c in range(3):
        for n in range(g.lead):
            out[0, c, n] = ref[c, n, 2:4, :]
            out[1, c, n] = ref[c, n, g.sub : g.sub + 2, :]


def unpack_sub(g, ext, got):
    ref = ext[1 - g.lead_axis]
    for c in range(3):
        for n in range(g.lead):
            ref[c, n, 0:2, :] = got[0, c, n]
            ref[c, n, 2 + g.sub : 4 + g.sub, :] = got[1, c, n]


def pack_y(grids, exts, out):
    for tile, (g, ext) in enumerate(zip(grids, exts)):
        lane = lax.broadcasted_iota(jnp.int32, (g.sub, 128), 1)
        total = jnp.zeros((g.sub, 128), jnp.float32)
        for c in range(3):
            for n in range(g.lead):
                i = c * g.lead + n
                plane = ext[2][c, n, :, 0:128]
                if g.ny > 128:
                    plane = jnp.where(lane < 64, plane, ext[2][c, n, :, g.ny - 128 : g.ny])
                total = jnp.where(lane // 4 == i, roll(plane, 4 * i + 2, 1), total)
        out[tile, 0 : g.sub, :] = total


def unpack_y(grids, exts, got):
    for tile, (g, ext) in enumerate(zip(grids, exts)):
        lane = lax.broadcasted_iota(jnp.int32, (g.sub, 128), 1)
        both = jnp.where(lane % 4 < 2, got[0, tile, 0 : g.sub, :], got[1, tile, 0 : g.sub, :])
        for c in range(3):
            for n in range(g.lead):
                i = c * g.lead + n
                ext[2][c, n, :, g.ny : g.ny + 128] = roll(both, -(4 * i + 2), 1)


def couple(fine, coarse, fext, cext):
    fz, cz = fext[0], cext[0]
    nt = fine.ny // 128
    rows = fz.shape[2]
    lane = lax.broadcasted_iota(jnp.int32, (rows, 128), 1)
    clane = lane[0 : coarse.sub]
    last = 1 + fine.sub
    for c in range(3):
        plane = cz[c, 2]
        spread = jnp.concatenate(
            [jnp.take_along_axis(plane, (clane + 128 * t) // 3, axis=1) for t in range(nt)], axis=1
        )
        for n in range(fine.lead):
            bottom = fz[c, n, last : last + 1, :]
            row = spread[n // 3 : n // 3 + 1]
            fz[c, n, last + 1 : last + 2, :] = 2.0 / 3.0 * bottom + 1.0 / 3.0 * row
            fz[c, n, last + 2 : last + 3, :] = 1.0 / 3.0 * bottom + 2.0 / 3.0 * row
        for r in range(coarse.sub):
            f = fz[c, 3 * r] + fz[c, 3 * r + 1] + fz[c, 3 * r + 2]
            f = f + roll(f, -1, 1) + roll(f, -2, 1)
            out = jnp.zeros((rows, 128), jnp.float32)
            for t in range(nt):
                got = jnp.take_along_axis(f[:, 128 * t : 128 * t + 128], (3 * lane) % 128, axis=1)
                out = jnp.where((3 * lane) // 128 == t, got, out)
            out = out * (1.0 / 9.0)
            cz[c, 1, r : r + 1, :] = out[last : last + 1]
            cz[c, 0, r : r + 1, :] = out[last - 3 : last - 2]


def materials(g, zones, tables, out):
    def body(z, carry):
        ids = zones[g.at(z)]
        values = [jnp.zeros(ids.shape, jnp.float32)] * 3
        for member in range(tables[0].shape[0]):
            hit = ids == member
            values = [jnp.where(hit, t[member], v) for t, v in zip(tables, values)]
        out[0, z] = DT * values[0]
        out[1, z] = DT * values[1]
        out[2, z] = DT * values[2]
        return carry

    lax.fori_loop(0, g.lead, body, 0)


def velocity_update(g, sext, vext, mats, velocity):
    allc = (0, 1, 2)

    def body(z, carry):
        b = mats[0, z]
        force = (
            diff(g, 1, sext, 0, z, True) + diff(g, 2, sext, 1, z, False) + diff(g, 0, sext, 1, z, False),
            diff(g, 1, sext, 1, z, False) + diff(g, 2, sext, 0, z, True) + diff(g, 0, sext, 2, z, False),
            diff(g, 1, sext, 2, z, False) + diff(g, 2, sext, 2, z, False) + diff(g, 0, sext, 0, z, True),
        )
        new = [velocity[c, g.at(z)] + b * force[c] for c in range(3)]
        for c in range(3):
            velocity[c, g.at(z)] = new[c]
        put_ext(g, vext, (allc, allc, allc), z, new)
        return carry

    lax.fori_loop(0, g.lead, body, 0)


def stress_update(g, vext, sext, mats, stress, iwan, last):

    def body(z, carry):
        lame, shear = mats[1, z], mats[2, z]
        exx = diff(g, 1, vext, 0, z, False)
        eyy = diff(g, 2, vext, 1, z, False)
        ezz = diff(g, 0, vext, 2, z, False)
        exy = diff(g, 1, vext, 1, z, True) + diff(g, 2, vext, 0, z, True)
        exz = diff(g, 1, vext, 2, z, True) + diff(g, 0, vext, 0, z, True)
        eyz = diff(g, 2, vext, 2, z, True) + diff(g, 0, vext, 1, z, True)
        dilation = exx + eyy + ezz
        old = [stress[c, g.at(z)] for c in range(6)]
        volume = lame * dilation
        twice = 2.0 * shear
        shears = [shear * exy, shear * exz, shear * eyz]
        new = [old[c] + volume + twice * e for c, e in enumerate((exx, eyy, ezz))]
        new += [old[3 + c] + shears[c] for c in range(3)]
        if iwan is not None:
            states, plastic, share, radius, surfaces = iwan
            third = dilation * (1.0 / 3.0)
            total = share[0]
            for k in range(1, surfaces):
                total = total + share[k]
            scale = 1.0 / jnp.full(dilation.shape, total, jnp.float32)
            dd = [scale * (twice * (e - third)) for e in (exx, eyy, ezz)]
            dd += [scale * s for s in shears]
            sums = None
            for k in range(surfaces):
                t = [states[k, c, z] + share[k] * dd[c] for c in range(6)]
                j2 = 0.5 * (t[0] * t[0] + t[1] * t[1] + t[2] * t[2]) + (
                    t[3] * t[3] + t[4] * t[4] + t[5] * t[5]
                )
                factor = jnp.minimum(1.0, radius[k] * lax.rsqrt(j2))
                t = [factor * x for x in t]
                if not last:
                    for c in range(6):
                        states[k, c, z] = t[c]
                sums = t if sums is None else [a + b for a, b in zip(sums, t)]
            mean = (old[0] + old[1] + old[2]) * (1.0 / 3.0) + (lame + twice * (1.0 / 3.0)) * dilation
            active = plastic[z] == 1
            yielded = [mean + sums[c] for c in range(3)] + sums[3:]
            new = [jnp.where(active, a, b) for a, b in zip(yielded, new)]
        for c in range(6):
            stress[c, g.at(z)] = new[c]
        if not last:
            put_ext(g, sext, (Z_PARTS, X_PARTS, Y_PARTS), z, new)
        return carry

    lax.fori_loop(0, g.lead, body, 0)


def kernel(counts, fine, coarse, surfaces, *refs):
    tables, share, radius = refs[8:11], refs[11], refs[12]
    outs = refs[13:17]
    (fv, fs, cv, cs, st, fzo, czo, plastic) = refs[17:25]
    fmat, cmat = refs[25:27]
    fsx, csx, fvx, cvx = refs[27:30], refs[30:33], refs[33:36], refs[36:39]
    fsub, csub, ysend, fsub_got, csub_got, ygot = refs[39:45]
    in_sem, out_sem, send_sem, recv_sem = refs[45:49]
    grids = (fine, coarse)

    place = [lax.axis_index(a) for a in AXES]
    exists = lambda a, side: (place[a] > 0) if side == 0 else (place[a] < counts[a] - 1)
    peer = lambda a, side: {AXES[a]: place[a] + (1 if side else -1)}

    loads = [
        pltpu.make_async_copy(src, dst, in_sem.at[i])
        for i, (src, dst) in enumerate(zip(refs[:8], refs[17:25]))
    ]
    for i in (1, 3, 0, 2, 5, 6, 7, 4):
        loads[i].start()

    def lead_face(g, ref, side, halo):
        low = 0 if halo else 2
        high = 2 + g.lead if halo else g.lead
        up = side if not g.flipped else 1 - side
        return ref.at[:, pl.ds(high if up else low, 2)]

    barrier = pltpu.get_barrier_semaphore()
    for a in range(3):
        for side in range(2):

            @pl.when(exists(a, side))
            def _():
                pl.semaphore_signal(barrier, inc=1, device_id=peer(a, side), device_id_type=MESH)

            @pl.when(jnp.logical_not(exists(a, side)))
            def _():
                if a == 2:
                    for e in range(2 * STEPS):
                        ygot[e, side] = jnp.zeros(ygot.shape[2:], jnp.float32)
                    return
                for g, ext, sub in (
                    (fine, fsx, fsub_got), (fine, fvx, None), (coarse, csx, csub_got), (coarse, cvx, None)
                ):
                    if a == g.lead_axis:
                        up = side if not g.flipped else 1 - side
                        at = 2 + g.lead if up else 0
                        for c in range(3):
                            for l in range(2):
                                ext[a][c, at + l] = jnp.zeros((g.sub, g.ny), jnp.float32)
                    elif sub is not None:
                        for e in range(2 * STEPS):
                            sub[e, side] = jnp.zeros(sub.shape[2:], jnp.float32)

    def copies(e, a, side):
        fext, cext = (fsx, csx) if e % 2 == 0 else (fvx, cvx)
        other = 1 - side
        if a == 2:
            pairs = [(ysend.at[e], ygot.at[e, other])]
        else:
            pairs = []
            for g, ext, sub, got in ((fine, fext, fsub, fsub_got), (coarse, cext, csub, csub_got)):
                if a == g.lead_axis:
                    pairs.append((lead_face(g, ext[a], side, False), lead_face(g, ext[a], other, True)))
                else:
                    pairs.append((sub.at[e, side], got.at[e, other]))
        return [
            pltpu.make_async_remote_copy(
                src_ref=src,
                dst_ref=dst,
                send_sem=send_sem.at[e, a, side, i],
                recv_sem=recv_sem.at[e, a, other, i],
                device_id=peer(a, side),
                device_id_type=MESH,
            )
            for i, (src, dst) in enumerate(pairs)
        ]

    def start(e, a):
        for side in range(2):

            @pl.when(exists(a, side))
            def _():
                for copy in copies(e, a, side):
                    copy.start()

    def arrive(e, a):
        for side in range(2):

            @pl.when(exists(a, side))
            def _():
                for copy in copies(e, a, 1 - side):
                    copy.wait_recv()

    def left(e):
        for a in range(3):
            for side in range(2):

                @pl.when(exists(a, side))
                def _():
                    for copy in copies(e, a, side):
                        copy.wait_send()

    parts = (Z_PARTS, X_PARTS, Y_PARTS)
    loads[1].wait()
    loads[3].wait()
    for g, s, ext in ((fine, fs, fsx), (coarse, cs, csx)):
        for n in range(g.lead):
            put_ext(g, ext, parts, n, [s[c, g.at(n)] for c in range(6)])

    at_interface = place[0] == counts[0] - 1
    for e in range(2 * STEPS):
        fext, cext = exts = (fsx, csx) if e % 2 == 0 else (fvx, cvx)
        pack_sub(coarse, cext, csub.at[e])
        if e == 0:
            neighbours = sum(
                exists(a, side).astype(jnp.int32) for a in range(3) for side in range(2)
            )
            pl.semaphore_wait(barrier, neighbours)
        start(e, 1)
        pack_sub(fine, fext, fsub.at[e])
        start(e, 0)
        pack_y(grids, exts, ysend.at[e])
        start(e, 2)
        if e == 0:
            loads[5].wait()
            loads[6].wait()
            materials(fine, fzo, tables, fmat)
            materials(coarse, czo, tables, cmat)
            loads[0].wait()
            loads[2].wait()
        arrive(e, 0)
        unpack_sub(fine, fext, fsub_got.at[e])

        @pl.when(at_interface)
        def _():
            couple(fine, coarse, fext, cext)

        arrive(e, 1)
        unpack_sub(coarse, cext, csub_got.at[e])
        arrive(e, 2)
        unpack_y(grids, exts, ygot.at[e])
        left(e)
        last = e >= 2 * STEPS - 2
        if e % 2 == 0:
            velocity_update(fine, fsx, fvx, fmat, fv)
            velocity_update(coarse, csx, cvx, cmat, cv)
            if last:
                stores = [
                    pltpu.make_async_copy(fv, outs[0], out_sem.at[0]),
                    pltpu.make_async_copy(cv, outs[2], out_sem.at[1]),
                ]
                for s in stores:
                    s.start()
        else:
            if e == 1:
                loads[7].wait()
                loads[4].wait()
            stress_update(
                fine, fvx, fsx, fmat, fs, (st, plastic, share, radius, surfaces), last
            )
            stress_update(coarse, cvx, csx, cmat, cs, None, last)
    tail = [
        pltpu.make_async_copy(fs, outs[1], out_sem.at[2]),
        pltpu.make_async_copy(cs, outs[3], out_sem.at[3]),
    ]
    for s in tail:
        s.start()
    for s in stores + tail:
        s.wait()


def swap(x):
    return jnp.swapaxes(x, -3, -2)


def per_device(counts, *args):
    args = [swap(x) if i in (0, 1, 4, 5, 7) else x for i, x in enumerate(args)]
    fv, fs, cv, cs, st = args[:5]
    fine = Grid(fv.shape[1:], 1.0, False, 1)
    coarse = Grid(cv.shape[1:], 3.0, True, 0)
    f32 = jnp.float32

    def exts(g):
        lead = pltpu.VMEM((3, g.lead + 4, g.sub, g.ny), f32)
        sub = pltpu.VMEM((3, g.lead, -(-(g.sub + 4) // 8) * 8, g.ny), f32)
        return [
            lead if g.lead_axis == 0 else sub,
            lead if g.lead_axis == 1 else sub,
            pltpu.VMEM((3, g.lead, g.sub, g.ny + 128), f32),
        ]

    phases = 2 * STEPS
    subs = [pltpu.VMEM((phases, 2, 3, g.lead, 2, g.ny), f32) for g in (fine, coarse)]
    scratch = [pltpu.VMEM(a.shape, a.dtype) for a in args[:8]]
    scratch += [pltpu.VMEM((3, g.lead, g.sub, g.ny), f32) for g in (fine, coarse)]
    scratch += exts(fine) + exts(coarse) + exts(fine) + exts(coarse)
    scratch += subs + [pltpu.VMEM((phases, 2, 8, 128), f32)]
    scratch += subs + [pltpu.VMEM((phases, 2, 2, 8, 128), f32)]
    scratch += [
        pltpu.SemaphoreType.DMA((8,)),
        pltpu.SemaphoreType.DMA((4,)),
        pltpu.SemaphoreType.DMA((phases, 3, 2, 2)),
        pltpu.SemaphoreType.DMA((phases, 3, 2, 2)),
    ]
    anywhere = pl.BlockSpec(memory_space=pl.ANY)
    scalars = pl.BlockSpec(memory_space=pltpu.SMEM)
    out = pl.pallas_call(
        lambda *refs: kernel(counts, fine, coarse, st.shape[0], *refs),
        name="waves",
        out_shape=[jax.ShapeDtypeStruct(a.shape, a.dtype) for a in (fv, fs, cv, cs)],
        in_specs=[anywhere] * 8 + [scalars] * 5,
        out_specs=[anywhere] * 4,
        scratch_shapes=scratch,
        compiler_params=pltpu.CompilerParams(collective_id=0, has_side_effects=True),
    )(*args)
    return swap(out[0]), swap(out[1]), out[2], out[3]


def solution(mesh):
    field = P(None, *AXES)
    cells = P(*AXES)
    counts = tuple(mesh.shape[a] for a in AXES)
    return jax.shard_map(
        lambda *args: per_device(counts, *args),
        mesh=mesh,
        in_specs=(field,) * 4 + (P(None, None, *AXES),) + (cells,) * 3 + (P(),) * 5,
        out_specs=(field,) * 4,
        check_vma=False,
    )
```

```python
import jax
import jax.numpy as jnp
from jax import lax
from jax.experimental import pallas as pl
from jax.experimental.pallas import tpu as pltpu
from jax.sharding import PartitionSpec as P

STEPS = 2
DT = 0.4
NEAR = 9.0 / 8.0
FAR = 1.0 / 24.0
MESH = pl.DeviceIdType.MESH
Z_PARTS, X_PARTS, Y_PARTS = (2, 4, 5), (0, 3, 4), (1, 3, 5)
AXES = ("depth", "hx", "hy")


class Grid:
    def __init__(self, shape, spacing, flipped, lead):
        self.lead, self.sub, self.ny = shape
        self.near, self.far = NEAR / spacing, FAR / spacing
        self.flipped = flipped
        self.lead_axis = lead

    def at(self, n):
        return self.lead - 1 - n if self.flipped else n


def roll(x, amount, axis):
    return pltpu.roll(x, amount % x.shape[axis], axis)


def diff(g, axis, ext, c, n, forward):
    ref = ext[axis]
    if axis == 2:
        full = ref[c, n]
        at = lambda s: (roll(full, -s, 1) if s else full)[:, : g.ny]
        o = 0
    elif axis == g.lead_axis:
        at = lambda s: ref[c, s]
        o = 2 + n
    else:
        at = lambda s: ref[c, n, s : s + g.sub, :]
        o = 2
    o = o + 1 if forward else o
    return g.near * (at(o) - at(o - 1)) - g.far * (at(o + 1) - at(o - 2))


def put_ext(g, ext, comps, n, values):
    for axis in range(3):
        for slot, c in enumerate(comps[axis]):
            if axis == 2:
                ext[axis][slot, n, :, : g.ny] = values[c]
            elif axis == g.lead_axis:
                ext[axis][slot, 2 + n] = values[c]
            else:
                ext[axis][slot, n, 2 : 2 + g.sub, :] = values[c]


def pack_sub(g, ext, out):
    ref = ext[1 - g.lead_axis]
    for c in range(3):
        for n in range(g.lead):
            out[0, c, n] = ref[c, n, 2:4, :]
            out[1, c, n] = ref[c, n, g.sub : g.sub + 2, :]


def unpack_sub(g, ext, got):
    ref = ext[1 - g.lead_axis]
    for c in range(3):
        for n in range(g.lead):
            ref[c, n, 0:2, :] = got[0, c, n]
            ref[c, n, 2 + g.sub : 4 + g.sub, :] = got[1, c, n]


def pack_y(grids, exts, out):
    for tile, (g, ext) in enumerate(zip(grids, exts)):
        lane = lax.broadcasted_iota(jnp.int32, (g.sub, 128), 1)
        total = jnp.zeros((g.sub, 128), jnp.float32)
        for c in range(3):
            for n in range(g.lead):
                i = c * g.lead + n
                plane = ext[2][c, n, :, 0:128]
                if g.ny > 128:
                    plane = jnp.where(lane < 64, plane, ext[2][c, n, :, g.ny - 128 : g.ny])
                total = jnp.where(lane // 4 == i, roll(plane, 4 * i + 2, 1), total)
        out[tile, 0 : g.sub, :] = total


def unpack_y(grids, exts, got):
    for tile, (g, ext) in enumerate(zip(grids, exts)):
        lane = lax.broadcasted_iota(jnp.int32, (g.sub, 128), 1)
        both = jnp.where(lane % 4 < 2, got[0, tile, 0 : g.sub, :], got[1, tile, 0 : g.sub, :])
        for c in range(3):
            for n in range(g.lead):
                i = c * g.lead + n
                ext[2][c, n, :, g.ny : g.ny + 128] = roll(both, -(4 * i + 2), 1)


def couple(fine, coarse, fext, cext):
    fz, cz = fext[0], cext[0]
    nt = fine.ny // 128
    rows = fz.shape[2]
    lane = lax.broadcasted_iota(jnp.int32, (rows, 128), 1)
    clane = lane[0 : coarse.sub]
    last = 1 + fine.sub
    for c in range(3):
        plane = cz[c, 2]
        spread = jnp.concatenate(
            [jnp.take_along_axis(plane, (clane + 128 * t) // 3, axis=1) for t in range(nt)], axis=1
        )
        for n in range(fine.lead):
            bottom = fz[c, n, last : last + 1, :]
            row = spread[n // 3 : n // 3 + 1]
            fz[c, n, last + 1 : last + 2, :] = 2.0 / 3.0 * bottom + 1.0 / 3.0 * row
            fz[c, n, last + 2 : last + 3, :] = 1.0 / 3.0 * bottom + 2.0 / 3.0 * row
        for r in range(coarse.sub):
            f = fz[c, 3 * r] + fz[c, 3 * r + 1] + fz[c, 3 * r + 2]
            f = f + roll(f, -1, 1) + roll(f, -2, 1)
            out = jnp.zeros((rows, 128), jnp.float32)
            for t in range(nt):
                got = jnp.take_along_axis(f[:, 128 * t : 128 * t + 128], (3 * lane) % 128, axis=1)
                out = jnp.where((3 * lane) // 128 == t, got, out)
            out = out * (1.0 / 9.0)
            cz[c, 1, r : r + 1, :] = out[last : last + 1]
            cz[c, 0, r : r + 1, :] = out[last - 3 : last - 2]


def materials(g, zones, tables, out):
    def body(z, carry):
        ids = zones[g.at(z)]
        values = [jnp.zeros(ids.shape, jnp.float32)] * 3
        for member in range(tables[0].shape[0]):
            hit = ids == member
            values = [jnp.where(hit, t[member], v) for t, v in zip(tables, values)]
        out[0, z] = DT * values[0]
        out[1, z] = DT * values[1]
        out[2, z] = DT * values[2]
        return carry

    lax.fori_loop(0, g.lead, body, 0)


class Planes:
    def __init__(self, g, kind):
        self.kind, self.lead = kind, g.lead
        self.count = {"all": g.lead, "inner": g.lead - 4, "outer": 4}[kind]

    def __call__(self, i):
        if self.kind == "outer":
            return i + (i // 2) * (self.lead - 4)
        return i + 2 if self.kind == "inner" else i


def velocity_update(g, sext, vext, mats, velocity, out, planes):
    allc = (0, 1, 2)

    def body(i, carry):
        z = planes(i)
        b = mats[0, z]
        force = (
            diff(g, 1, sext, 0, z, True) + diff(g, 2, sext, 1, z, False) + diff(g, 0, sext, 1, z, False),
            diff(g, 1, sext, 1, z, False) + diff(g, 2, sext, 0, z, True) + diff(g, 0, sext, 2, z, False),
            diff(g, 1, sext, 2, z, False) + diff(g, 2, sext, 2, z, False) + diff(g, 0, sext, 0, z, True),
        )
        new = [velocity[c, g.at(z)] + b * force[c] for c in range(3)]
        for c in range(3):
            out[c, g.at(z)] = new[c]
        put_ext(g, vext, (allc, allc, allc), z, new)
        return carry

    lax.fori_loop(0, planes.count, body, 0)


def stress_update(g, vext, sext, mats, stress, out, iwan, last, planes):

    def body(i, carry):
        z = planes(i)
        lame, shear = mats[1, z], mats[2, z]
        exx = diff(g, 1, vext, 0, z, False)
        eyy = diff(g, 2, vext, 1, z, False)
        ezz = diff(g, 0, vext, 2, z, False)
        exy = diff(g, 1, vext, 1, z, True) + diff(g, 2, vext, 0, z, True)
        exz = diff(g, 1, vext, 2, z, True) + diff(g, 0, vext, 0, z, True)
        eyz = diff(g, 2, vext, 2, z, True) + diff(g, 0, vext, 1, z, True)
        dilation = exx + eyy + ezz
        old = [stress[c, g.at(z)] for c in range(6)]
        volume = lame * dilation
        twice = 2.0 * shear
        shears = [shear * exy, shear * exz, shear * eyz]
        new = [old[c] + volume + twice * e for c, e in enumerate((exx, eyy, ezz))]
        new += [old[3 + c] + shears[c] for c in range(3)]
        if iwan is not None:
            states, plastic, share, radius, surfaces = iwan
            third = dilation * (1.0 / 3.0)
            total = share[0]
            for k in range(1, surfaces):
                total = total + share[k]
            scale = 1.0 / jnp.full(dilation.shape, total, jnp.float32)
            dd = [scale * (twice * (e - third)) for e in (exx, eyy, ezz)]
            dd += [scale * s for s in shears]
            sums = None
            for k in range(surfaces):
                t = [states[k, c, z] + share[k] * dd[c] for c in range(6)]
                j2 = 0.5 * (t[0] * t[0] + t[1] * t[1] + t[2] * t[2]) + (
                    t[3] * t[3] + t[4] * t[4] + t[5] * t[5]
                )
                factor = jnp.minimum(1.0, radius[k] * lax.rsqrt(j2))
                t = [factor * x for x in t]
                if not last:
                    for c in range(6):
                        states[k, c, z] = t[c]
                sums = t if sums is None else [a + b for a, b in zip(sums, t)]
            mean = (old[0] + old[1] + old[2]) * (1.0 / 3.0) + (lame + twice * (1.0 / 3.0)) * dilation
            active = plastic[z] == 1
            yielded = [mean + sums[c] for c in range(3)] + sums[3:]
            new = [jnp.where(active, a, b) for a, b in zip(yielded, new)]
        for c in range(6):
            out[c, g.at(z)] = new[c]
        if not last:
            put_ext(g, sext, (Z_PARTS, X_PARTS, Y_PARTS), z, new)
        return carry

    lax.fori_loop(0, planes.count, body, 0)


def kernel(counts, fine, coarse, surfaces, *refs):
    tables, share, radius = refs[48:51], refs[51], refs[52]
    outs = refs[13:17]
    (fv, fs, cv, cs, st, fzo, czo, plastic) = refs[17:25]
    fmat, cmat = refs[25:27]
    fsx, csx, fvx, cvx = refs[27:30], refs[30:33], refs[33:36], refs[36:39]
    fsub, csub, ysend, fsub_got, csub_got, ygot = refs[39:45]
    in_sem, send_sem, recv_sem = refs[45:48]
    grids = (fine, coarse)

    place = [lax.axis_index(a) for a in AXES]
    exists = lambda a, side: (place[a] > 0) if side == 0 else (place[a] < counts[a] - 1)
    peer = lambda a, side: {AXES[a]: place[a] + (1 if side else -1)}

    loads = [
        pltpu.make_async_copy(src, dst, in_sem.at[i])
        for i, (src, dst) in enumerate(zip(refs[:8], refs[17:25]))
    ]
    scalars = [
        pltpu.make_async_copy(src, dst, in_sem.at[8 + i])
        for i, (src, dst) in enumerate(zip(refs[8:13], refs[48:53]))
    ]

    for i in (1, 3):
        loads[i].start()

    def lead_face(g, ref, side, halo):
        low = 0 if halo else 2
        high = 2 + g.lead if halo else g.lead
        up = side if not g.flipped else 1 - side
        return ref.at[:, pl.ds(high if up else low, 2)]

    barrier = pltpu.get_barrier_semaphore()
    for a in range(3):
        for side in range(2):

            @pl.when(exists(a, side))
            def _():
                pl.semaphore_signal(barrier, inc=1, device_id=peer(a, side), device_id_type=MESH)

            @pl.when(jnp.logical_not(exists(a, side)))
            def _():
                if a == 2:
                    for e in range(2 * STEPS):
                        ygot[e, side] = jnp.zeros(ygot.shape[2:], jnp.float32)
                    return
                for g, ext, sub in (
                    (fine, fsx, fsub_got), (fine, fvx, None), (coarse, csx, csub_got), (coarse, cvx, None)
                ):
                    if a == g.lead_axis:
                        up = side if not g.flipped else 1 - side
                        at = 2 + g.lead if up else 0
                        for c in range(3):
                            for l in range(2):
                                ext[a][c, at + l] = jnp.zeros((g.sub, g.ny), jnp.float32)
                    elif sub is not None:
                        for e in range(2 * STEPS):
                            sub[e, side] = jnp.zeros(sub.shape[2:], jnp.float32)

    for copy in [loads[i] for i in (0, 2, 5, 6)] + scalars + [loads[7], loads[4]]:
        copy.start()

    def copies(e, a, side):
        fext, cext = (fsx, csx) if e % 2 == 0 else (fvx, cvx)
        other = 1 - side
        if a == 2:
            pairs = [(ysend.at[e], ygot.at[e, other])]
        else:
            pairs = []
            for g, ext, sub, got in ((fine, fext, fsub, fsub_got), (coarse, cext, csub, csub_got)):
                if a == g.lead_axis:
                    pairs.append((lead_face(g, ext[a], side, False), lead_face(g, ext[a], other, True)))
                else:
                    pairs.append((sub.at[e, side], got.at[e, other]))
        return [
            pltpu.make_async_remote_copy(
                src_ref=src,
                dst_ref=dst,
                send_sem=send_sem.at[e, a, side, i],
                recv_sem=recv_sem.at[e, a, other, i],
                device_id=peer(a, side),
                device_id_type=MESH,
            )
            for i, (src, dst) in enumerate(pairs)
        ]

    def start(e, a):
        for side in range(2):

            @pl.when(exists(a, side))
            def _():
                for copy in copies(e, a, side):
                    copy.start()

    def arrive(e, a):
        for side in range(2):

            @pl.when(exists(a, side))
            def _():
                for copy in copies(e, a, 1 - side):
                    copy.wait_recv()

    def left(e):
        for a in range(3):
            for side in range(2):

                @pl.when(exists(a, side))
                def _():
                    for copy in copies(e, a, side):
                        copy.wait_send()

    parts = (Z_PARTS, X_PARTS, Y_PARTS)
    loads[1].wait()
    loads[3].wait()
    for g, s, ext in ((fine, fs, fsx), (coarse, cs, csx)):
        for n in range(g.lead):
            put_ext(g, ext, parts, n, [s[c, g.at(n)] for c in range(6)])

    at_interface = place[0] == counts[0] - 1
    for e in range(2 * STEPS):
        fext, cext = exts = (fsx, csx) if e % 2 == 0 else (fvx, cvx)
        pack_sub(coarse, cext, csub.at[e])
        if e == 0:
            neighbours = sum(
                exists(a, side).astype(jnp.int32) for a in range(3) for side in range(2)
            )
            pl.semaphore_wait(barrier, neighbours)
        start(e, 1)
        pack_sub(fine, fext, fsub.at[e])
        start(e, 0)
        pack_y(grids, exts, ysend.at[e])
        start(e, 2)
        if e == 0:
            loads[5].wait()
            loads[6].wait()
            for copy in scalars:
                copy.wait()
            materials(fine, fzo, tables, fmat)
            materials(coarse, czo, tables, cmat)
            loads[0].wait()
            loads[2].wait()
        arrive(e, 0)
        unpack_sub(fine, fext, fsub_got.at[e])

        @pl.when(at_interface)
        def _():
            couple(fine, coarse, fext, cext)

        arrive(e, 2)
        unpack_y(grids, exts, ygot.at[e])
        if e:
            left(e - 1)
        last = e >= 2 * STEPS - 2
        if e == 1:
            loads[7].wait()
            loads[4].wait()

        def update(planes):
            if e % 2 == 0:
                velocity_update(fine, fsx, fvx, fmat, fv, outs[0] if last else fv, planes)
            else:
                iwan = (st, plastic, share, radius, surfaces)
                stress_update(fine, fvx, fsx, fmat, fs, outs[1] if last else fs, iwan, last, planes)

        update(Planes(fine, "inner"))
        arrive(e, 1)
        unpack_sub(coarse, cext, csub_got.at[e])
        update(Planes(fine, "outer"))
        if e % 2 == 0:
            velocity_update(coarse, csx, cvx, cmat, cv, outs[2] if last else cv, Planes(coarse, "all"))
        else:
            stress_update(coarse, cvx, csx, cmat, cs, outs[3] if last else cs, None, last, Planes(coarse, "all"))
    left(2 * STEPS - 1)


def swap(x):
    return jnp.swapaxes(x, -3, -2)


def hand_over(*refs):
    copies = [pltpu.make_async_copy(refs[i], refs[4 + i], refs[8].at[i]) for i in range(4)]
    for copy in copies:
        copy.start()
    for copy in copies:
        copy.wait()


def per_device(counts, *args):
    args = [swap(x) if i in (0, 1, 4, 5, 7) else x for i, x in enumerate(args)]
    fv, fs, cv, cs, st = args[:5]
    fine = Grid(fv.shape[1:], 1.0, False, 1)
    coarse = Grid(cv.shape[1:], 3.0, True, 0)
    f32 = jnp.float32

    def exts(g):
        lead = pltpu.VMEM((3, g.lead + 4, g.sub, g.ny), f32)
        sub = pltpu.VMEM((3, g.lead, -(-(g.sub + 4) // 8) * 8, g.ny), f32)
        return [
            lead if g.lead_axis == 0 else sub,
            lead if g.lead_axis == 1 else sub,
            pltpu.VMEM((3, g.lead, g.sub, g.ny + 128), f32),
        ]

    phases = 2 * STEPS
    subs = [pltpu.VMEM((phases, 2, 3, g.lead, 2, g.ny), f32) for g in (fine, coarse)]
    scratch = [pltpu.VMEM(a.shape, a.dtype) for a in args[:8]]
    scratch += [pltpu.VMEM((3, g.lead, g.sub, g.ny), f32) for g in (fine, coarse)]
    scratch += exts(fine) + exts(coarse) + exts(fine) + exts(coarse)
    scratch += subs + [pltpu.VMEM((phases, 2, 8, 128), f32)]
    scratch += subs + [pltpu.VMEM((phases, 2, 2, 8, 128), f32)]
    scratch += [
        pltpu.SemaphoreType.DMA((13,)),
        pltpu.SemaphoreType.DMA((phases, 3, 2, 2)),
        pltpu.SemaphoreType.DMA((phases, 3, 2, 2)),
    ]
    scratch += [pltpu.SMEM(a.shape, a.dtype) for a in args[8:]]
    anywhere = pl.BlockSpec(memory_space=pl.ANY)
    out = pl.pallas_call(
        lambda *refs: kernel(counts, fine, coarse, st.shape[0], *refs),
        name="waves",
        out_shape=[pltpu.VMEM(a.shape, a.dtype) for a in (fv, fs, cv, cs)],
        in_specs=[pl.BlockSpec(memory_space=pltpu.HBM)] * 13,
        out_specs=[pl.BlockSpec(memory_space=pltpu.VMEM)] * 4,
        scratch_shapes=scratch,
        compiler_params=pltpu.CompilerParams(
            collective_id=0, has_side_effects=True
        ),
    )(*args)
    out = pl.pallas_call(
        hand_over,
        name="results",
        out_shape=[jax.ShapeDtypeStruct(a.shape, a.dtype) for a in (fv, fs, cv, cs)],
        in_specs=[anywhere] * 4,
        out_specs=[anywhere] * 4,
        scratch_shapes=[pltpu.SemaphoreType.DMA((4,))],
        compiler_params=pltpu.CompilerParams(vmem_limit_bytes=4 << 20),
    )(*out)
    return swap(out[0]), swap(out[1]), out[2], out[3]


def solution(mesh):
    field = P(None, *AXES)
    cells = P(*AXES)
    counts = tuple(mesh.shape[a] for a in AXES)
    return jax.shard_map(
        lambda *args: per_device(counts, *args),
        mesh=mesh,
        in_specs=(field,) * 4 + (P(None, None, *AXES),) + (cells,) * 3 + (P(),) * 5,
        out_specs=(field,) * 4,
        check_vma=False,
    )
```
